32 devices in a mesh: band: 4 (over y, x), grid: 8 (over z, core).
Axes of the slice: x: 2, y: 2, z: 4, core: 2. Of those that a mesh axis runs over, the one named last changes fastest.
Arguments:
- wavefunctions: bfloat16 [1024, 131072], P('band', 'grid'), may hold values from -6 to 6
- projectors: bfloat16 [512, 8, 13, 256], P('grid'), may hold values from -0.0068359375 to 0.0068359375
- slot_atom: int32 [512, 8], P('grid'), may hold values from -1 to 255, as said below
- occupations: float32 [1024], P('band'), may hold values from 0.02 to 2
Outputs:
- density: float32 [256, 13, 13], P('grid')
The draws below stay inside these ranges and needn't reach their ends.
Inputs may be any that keep to these rules, and one draw needn't show every extreme that they name: `slot_atom`: -1 marks an empty slot. Any other entry is an atom a whose owning domain a // 32 lies within 3 domains, counted around the closed cycle of 8 domains, of the domain of the block, block index // 64. In every domain some block has all 8 slots filled.
All inputs are finite; a program needn't handle non-finite values.
Results may differ from the reference program's by a relative error of at most 0.0003.
Values sent between devices are 32-bit elements; how exact they have to be, the bound alone decides.
A program may use at most 64 MiB of HBM per device.

```python
import math
import jax
import jax.numpy as jnp
from jax import lax

NPROJ = 13
BLK = 256
CAP = 8
REACH = 3
NBLK = 64
ATOMS_DEV = 32
BANDS = 1024
ATOMS = 256
BLOCKS = 512
POINTS = 131072
N_GRID = 8


def draw_slot_atom(key, part):
    keys = jax.random.split(jax.random.fold_in(key, 71), 6)
    domain = jnp.arange(BLOCKS, dtype=jnp.int32) // NBLK
    lowest = max(CAP // 3, 1)
    crowding = jax.random.randint(keys[0], (N_GRID,), lowest, CAP + 1)
    filled = jax.random.randint(keys[1], (BLOCKS,), 0, 1 << 20) % crowding[domain] + 1
    full_block = jax.random.randint(keys[2], (N_GRID,), 0, NBLK)
    is_full = jnp.arange(BLOCKS, dtype=jnp.int32) % NBLK == full_block[domain]
    filled = jnp.where(is_full, CAP, filled)
    scores = jax.random.randint(keys[3], (BLOCKS, CAP), 0, 1 << 16) * CAP + jnp.arange(CAP, dtype=jnp.int32)[None, :]
    ranking = jnp.argsort(jnp.argsort(scores, axis=1), axis=1)
    used = ranking < filled[:, None]
    offset = jax.random.randint(keys[4], (BLOCKS, CAP), -REACH, REACH + 1)
    owner = jnp.mod(domain[:, None] + offset, N_GRID)
    local_atom = jax.random.randint(keys[5], (BLOCKS, CAP), 0, ATOMS_DEV)
    return jnp.where(used, owner * ATOMS_DEV + local_atom, -1).astype(jnp.int32)


def block_levels(own_key, shape, shards, low, largest):
    def one(position, shards_of):
        heights = jax.random.uniform(jax.random.fold_in(jax.random.fold_in(own_key, 6), position), (shards_of,), jnp.float32, low / len(shards), largest / len(shards))
        return jnp.repeat(jnp.exp(heights), shape[position] // shards_of).reshape((-1,) + (1,) * (len(shape) - position - 1))

    gain = one(*shards[0])
    for cut in shards[1:]:
        gain = gain * one(*cut)
    return gain


def gaussian(rng, extent, deviation, bound, shards=(), kind=jnp.bfloat16):
    level = block_levels(rng, extent, shards, -0.22, 0.18) if shards else 1.0
    array = jax.random.normal(rng, extent, jnp.float32) * deviation * level
    return jnp.minimum(jnp.maximum(array, -bound), bound).astype(kind)


def setup_inputs(seed: int = 0) -> dict:
    seeds = jax.random.split(jax.random.key(seed), 5)
    wavefunctions = gaussian(seeds[0], (BANDS, POINTS), 1.0, 6.0, ((0, 4), (1, 8)))
    projectors = gaussian(seeds[1], (BLOCKS, CAP, NPROJ, BLK), (BANDS * NBLK * CAP * BLK // (6 * ATOMS_DEV)) ** -0.5, 0.0068359375, ((0, 8),))
    slot_atom = draw_slot_atom(jax.random.fold_in(seeds[4], 71), 0)
    occupations = jnp.clip(jnp.exp(math.log(2.0) - 4.6051702 * jax.random.uniform(seeds[3], (BANDS,), jnp.float32) ** block_levels(seeds[3], (BANDS,), ((0, 4),), -0.2, 0.2)), 0.02, 2.0)
    return dict(wavefunctions=wavefunctions, projectors=projectors, slot_atom=slot_atom, occupations=occupations)


def reference(wavefunctions, projectors, slot_atom, occupations):
    band_total = wavefunctions.shape[0]
    domain_points = NBLK * BLK

    def domain_step(running, domain):
        columns = lax.dynamic_slice_in_dim(wavefunctions, (domain * domain_points).astype(jnp.int32), domain_points, 1)
        pieces = lax.dynamic_slice_in_dim(projectors, (domain * NBLK).astype(jnp.int32), NBLK, 0)
        slot_ids = lax.dynamic_slice_in_dim(slot_atom, (domain * NBLK).astype(jnp.int32), NBLK, 0).reshape(-1)
        grid_blocks = columns.astype(jnp.float32).reshape(band_total, NBLK, BLK)
        stacked = pieces.astype(jnp.float32).reshape(NBLK, CAP * NPROJ, BLK)
        slot_terms = jnp.einsum("ngb,gcb->gcn", grid_blocks, stacked, precision=lax.Precision.HIGHEST)
        slot_terms = slot_terms.reshape(NBLK * CAP, NPROJ * band_total)
        target = jnp.where(slot_ids >= 0, slot_ids, ATOMS).astype(jnp.int32)
        running = running + jax.ops.segment_sum(slot_terms, target, num_segments=ATOMS + 1)
        return running, None

    initial = jnp.zeros((ATOMS + 1, NPROJ * band_total), jnp.float32)
    running, unused = lax.scan(domain_step, initial, jnp.arange(N_GRID, dtype=jnp.int32))
    projections = running[:ATOMS].reshape(ATOMS, NPROJ, band_total)
    weighted = projections * occupations.reshape(1, 1, band_total)
    return jnp.einsum("ain,ajn->aij", weighted, projections, precision=lax.Precision.HIGHEST)
```

```python
import functools

import jax
import jax.numpy as jnp
from jax import lax
from jax.experimental import pallas as pl
from jax.experimental.pallas import tpu as pltpu
from jax.sharding import PartitionSpec as P

REACH = 3
ATOMS_DEV = 32
ROWS = 8
LANES = 128
STRIDE = 16
SKEW = 2
STEP_BLOCKS = 8
MESH = pl.DeviceIdType.MESH
HIGHEST = lax.Precision.HIGHEST


def nt_dot(a, b, precision=None):
    return lax.dot_general(
        a, b, (((1,), (1,)), ((), ())), precision=precision, preferred_element_type=jnp.float32
    )


def local_kernel(ids_ref, waves_ref, pieces_ref, out_ref, slots, padded):
    step = pl.program_id(0)
    per_step, capacity, proj_count, block_len = pieces_ref.shape
    bands = waves_ref.shape[0]
    halves, _, targets, lanes = out_ref.shape
    height = padded.shape[2]

    @pl.when(step == 0)
    def _():
        padded[...] = jnp.zeros_like(padded)

    row = lax.broadcasted_iota(jnp.int32, (proj_count * capacity, capacity * height), 0)
    col = lax.broadcasted_iota(jnp.int32, (proj_count * capacity, capacity * height), 1)
    swap = (col == (row % capacity) * height + row // capacity).astype(jnp.bfloat16)
    for g in range(per_step):
        padded[g, :, :proj_count, :] = pieces_ref[g]
    for g in range(per_step):
        stacked = padded[g].reshape(capacity * height, block_len)
        ordered = jnp.dot(swap, stacked, preferred_element_type=jnp.float32).astype(jnp.bfloat16)
        terms = nt_dot(ordered, waves_ref[:, g * block_len:(g + 1) * block_len])
        start = pl.multiple_of((step * per_step + g) * capacity, capacity)
        for i in range(proj_count):
            slots[pl.ds(start, capacity), i * bands:(i + 1) * bands] = terms[i * capacity:(i + 1) * capacity]

    @pl.when(step == pl.num_programs(0) - 1)
    def _():
        slot_count = slots.shape[0]
        wanted = lax.broadcasted_iota(jnp.int32, (targets, slot_count), 0)
        pick = (wanted == ids_ref[...]).astype(jnp.bfloat16)
        for i in range(proj_count):
            full = slots[:, i * bands:(i + 1) * bands]
            high = full.astype(jnp.bfloat16)
            low = (full - high.astype(jnp.float32)).astype(jnp.bfloat16)
            total = jnp.dot(pick, high, preferred_element_type=jnp.float32)
            total += jnp.dot(pick, low, preferred_element_type=jnp.float32)
            for h in range(halves):
                out_ref[h, i] = total[:, h * lanes:(h + 1) * lanes]


def local_window(wavefunctions, projectors, slot_ids, targets):
    bands = wavefunctions.shape[0]
    blocks, capacity, proj_count, block_len = projectors.shape
    height = -(-proj_count // 16) * 16
    shape = (bands // LANES, proj_count, targets, LANES)
    return pl.pallas_call(
        local_kernel,
        grid=(blocks // STEP_BLOCKS,),
        in_specs=[
            pl.BlockSpec((1, blocks * capacity), lambda s: (0, 0)),
            pl.BlockSpec((bands, STEP_BLOCKS * block_len), lambda s: (0, s)),
            pl.BlockSpec((STEP_BLOCKS, capacity, proj_count, block_len), lambda s: (s, 0, 0, 0)),
        ],
        out_specs=pl.BlockSpec(shape, lambda s: (0, 0, 0, 0)),
        out_shape=jax.ShapeDtypeStruct(shape, jnp.float32),
        scratch_shapes=[
            pltpu.VMEM((blocks * capacity, proj_count * bands), jnp.float32),
            pltpu.VMEM((STEP_BLOCKS, capacity, height, block_len), jnp.bfloat16),
        ],
        compiler_params=pltpu.CompilerParams(vmem_limit_bytes=40 << 20),
    )(slot_ids.reshape(1, -1), wavefunctions, projectors)


def reduce_kernel(groups, band_size, win, occ, out_ref, pair_in, hop_in, summed, mine, peers, final, landed,
                  pair_send, pair_recv, hop_send, hop_recv, peer_send, peer_recv, last_send, last_recv):
    halves, proj_count, _, lanes = win.shape
    band = lax.axis_index("band")
    domain = lax.axis_index("grid")
    core = domain % 2
    chip = domain // 2
    chips = groups // 2
    turns = chips // 2
    subs = ATOMS_DEV // ROWS
    per_turn = subs * halves
    chunks = turns * per_turn
    top = (proj_count + 1) // 2 * ROWS
    rows = proj_count * ROWS

    barrier = pltpu.get_barrier_semaphore()
    partner = (band, chip * 2 + 1 - core)
    met = [partner]
    for r in range(1, chips):
        met.append((band, ((chip + r) % chips) * 2 + core))
    for r in range(1, band_size):
        met.append(((band + r) % band_size, domain))
    for other in met:
        pl.semaphore_signal(barrier, inc=1, device_id=other, device_id_type=MESH)

    def place(direction, k):
        block = k // halves
        turn = block // subs
        owner = turns - 1 - turn if direction == 0 else turns + turn
        return k % halves, pl.multiple_of(block * ROWS, ROWS), owner, block % subs

    def pair_copy(direction, k):
        half, at, owner, sub = place(direction, k)
        source = pl.multiple_of((owner * 2 + 1 - core) * ATOMS_DEV + sub * ROWS, ROWS)
        return pltpu.make_async_remote_copy(
            src_ref=win.at[half, :, pl.ds(source, ROWS), :],
            dst_ref=pair_in.at[direction, half, :, pl.ds(at, ROWS), :],
            send_sem=pair_send.at[direction, k], recv_sem=pair_recv.at[direction, k],
            device_id=partner, device_id_type=MESH,
        )

    def hop_copy(direction, k):
        half, at, _, _ = place(direction, k)
        following = chip - 1 if direction == 0 else chip + 1
        return pltpu.make_async_remote_copy(
            src_ref=summed.at[direction, half, :, pl.ds(at, ROWS), :],
            dst_ref=hop_in.at[direction, half, :, pl.ds(at, ROWS), :],
            send_sem=hop_send.at[direction, k], recv_sem=hop_recv.at[direction, k],
            device_id=(band, following * 2 + core), device_id_type=MESH,
        )

    def peer_copy(turn, r):
        return pltpu.make_async_remote_copy(
            src_ref=mine.at[turn], dst_ref=peers.at[turn, r - 1],
            send_sem=peer_send.at[turn, r - 1], recv_sem=peer_recv.at[turn, r - 1],
            device_id=((band + r) % band_size, domain), device_id_type=MESH,
        )

    def last_copy(direction, turn):
        owner = turns - 1 - turn if direction == 0 else turns + turn
        return pltpu.make_async_remote_copy(
            src_ref=final.at[turn], dst_ref=landed,
            send_sem=last_send.at[turn], recv_sem=last_recv,
            device_id=(band, owner * 2 + core), device_id_type=MESH,
        )

    def summed_peers(turn):
        total = mine[turn]
        for r in range(1, band_size):
            peer_copy(turn, r).wait_recv()
            total = total + peers[turn, r - 1]
        return total

    mine[...] = jnp.zeros_like(mine)
    pl.semaphore_wait(barrier, len(met))

    @pl.loop(0, chunks)
    def _(k):
        for direction in range(2):
            pair_copy(direction, k).start()

    def density(direction, k):
        half, at, _, sub = place(direction, k)
        x = summed[direction, half, :, pl.ds(at, ROWS), :].reshape(rows, lanes)
        gram = nt_dot(x * occ[half], x, HIGHEST)
        r = lax.broadcasted_iota(jnp.int32, (rows, rows), 0)
        c = lax.broadcasted_iota(jnp.int32, (rows, rows), 1)
        gram = jnp.where(r % ROWS == c % ROWS, gram, 0.0)
        j = lax.broadcasted_iota(jnp.int32, (rows, LANES), 0) // ROWS
        lane = lax.broadcasted_iota(jnp.int32, (rows, LANES), 1)
        upper = (lane == sub * STRIDE + j).astype(jnp.float32)
        lower = (lane == (subs + sub) * STRIDE + j).astype(jnp.float32)
        turn = k // per_turn
        mine[turn, :, :] += jnp.dot(gram[:top], upper, precision=HIGHEST, preferred_element_type=jnp.float32)
        mine[turn, :rows - top, :] += jnp.dot(gram[top:], lower, precision=HIGHEST, preferred_element_type=jnp.float32)
        for turn in range(turns):
            @pl.when(k == (turn + 1) * per_turn - 1)
            def _():
                for r in range(1, band_size):
                    peer_copy(turn, r).start()
        for turn in range(turns - 1):
            @pl.when(k == (turn + 1) * per_turn - 1 + per_turn // 2)
            def _():
                final[turn] = summed_peers(turn)
                last_copy(direction, turn).start()

    def process(direction, k, hops):
        half, at, owner, sub = place(direction, k)
        source = pl.multiple_of((owner * 2 + core) * ATOMS_DEV + sub * ROWS, ROWS)
        here = (direction, half, slice(None), pl.ds(at, ROWS), slice(None))
        pair_copy(direction, k).wait_recv()
        summed[here] = win[half, :, pl.ds(source, ROWS), :] + pair_in[here]

        @pl.when(hops > 0)
        def _():
            hop_copy(direction, k).wait_recv()
            summed[here] = summed[here] + hop_in[here]

        @pl.when(hops < chips - 1)
        def _():
            hop_copy(direction, k).start()

        @pl.when(hops == chips - 1)
        def _():
            density(direction, k)

    @pl.loop(0, chunks + SKEW * (chips - 1))
    def _(t):
        for direction in range(2):
            hops = chips - 1 - chip if direction == 0 else chip
            k = t - SKEW * hops

            @pl.when((k >= 0) & (k < chunks))
            def _():
                process(direction, k, hops)

    edge = (chip == 0) | (chip == chips - 1)

    @pl.when(edge)
    def _():
        out_ref[...] = summed_peers(turns - 1)
        for turn in range(turns):
            for r in range(1, band_size):
                peer_copy(turn, r).wait_send()
        for turn in range(turns - 1):
            last_copy(0, turn).wait_send()

    @pl.when(jnp.logical_not(edge))
    def _():
        last_copy(0, 0).wait_recv()
        out_ref[...] = landed[...]

    @pl.loop(0, chunks)
    def _(k):
        for direction in range(2):
            hops = chips - 1 - chip if direction == 0 else chip
            pair_copy(direction, k).wait_send()

            @pl.when(hops < chips - 1)
            def _():
                hop_copy(direction, k).wait_send()


def reduce_density(window, occupations, groups, band_size):
    halves, proj_count, _, lanes = window.shape
    turns = groups // 4
    chunks = turns * ATOMS_DEV // ROWS * halves
    top = (proj_count + 1) // 2 * ROWS
    handled = (2, halves, proj_count, turns * ATOMS_DEV, lanes)
    vmem = pl.BlockSpec(memory_space=pltpu.VMEM)
    dma = pltpu.SemaphoreType.DMA
    packed = pl.pallas_call(
        functools.partial(reduce_kernel, groups, band_size),
        in_specs=[vmem, vmem],
        out_specs=vmem,
        out_shape=jax.ShapeDtypeStruct((top, LANES), jnp.float32),
        scratch_shapes=[
            pltpu.VMEM(handled, jnp.float32),
            pltpu.VMEM(handled, jnp.float32),
            pltpu.VMEM(handled, jnp.float32),
            pltpu.VMEM((turns, top, LANES), jnp.float32),
            pltpu.VMEM((turns, band_size - 1, top, LANES), jnp.float32),
            pltpu.VMEM((turns, top, LANES), jnp.float32),
            pltpu.VMEM((top, LANES), jnp.float32),
            dma((2, chunks)), dma((2, chunks)), dma((2, chunks)), dma((2, chunks)),
            dma((turns, band_size - 1)), dma((turns, band_size - 1)), dma((turns,)), dma,
        ],
        compiler_params=pltpu.CompilerParams(
            collective_id=0, has_side_effects=True, vmem_limit_bytes=40 << 20
        ),
    )(window, occupations.reshape(halves, 1, lanes))
    subs = ATOMS_DEV // ROWS
    packed = packed.reshape(top // ROWS, ROWS, 2, subs, STRIDE).transpose(3, 1, 2, 0, 4)
    packed = packed.reshape(ATOMS_DEV, 2 * top // ROWS, STRIDE)
    return packed[:, :proj_count, :proj_count]


def shifted(block, axis, distance):
    devices = range(lax.axis_size(axis))
    route = [((i - distance) % len(devices), i) for i in devices]
    return lax.ppermute(block, axis, route)


def ring_density(wavefunctions, projectors, slot_ids, occupations):
    domains = lax.axis_size("grid")
    domain = lax.axis_index("grid")
    window_len = 2 * REACH + 1
    owner = jnp.floor_divide(slot_ids, ATOMS_DEV)
    offset = jnp.mod(owner - domain + REACH, domains)
    target = jnp.where(slot_ids >= 0, offset * ATOMS_DEV + jnp.mod(slot_ids, ATOMS_DEV), -1)
    window = local_window(wavefunctions, projectors, target, window_len * ATOMS_DEV)
    halves, proj_count, _, lanes = window.shape
    window = window.reshape(halves, proj_count, window_len, ATOMS_DEV, lanes)
    part = lambda at: window[:, :, at]
    forward = part(2 * REACH)
    for hop in range(REACH, 0, -1):
        forward = shifted(forward, "grid", 1) + part(REACH + hop - 1)
    backward = part(0)
    for hop in range(REACH, 0, -1):
        backward = shifted(backward, "grid", -1)
        if hop > 1:
            backward = backward + part(REACH - hop + 1)
    owned = forward + backward
    weighted = owned * occupations.reshape(halves, 1, 1, lanes)
    partial_sum = jnp.einsum("hian,hjan->aij", weighted, owned, precision=HIGHEST)
    return lax.psum(partial_sum, "band")


def body(wavefunctions, projectors, slot_atom, occupations):
    domains = lax.axis_size("grid")
    slot_ids = slot_atom.reshape(-1)
    if domains <= 2 * REACH + 2 and domains % 4 == 0:
        window = local_window(wavefunctions, projectors, slot_ids, domains * ATOMS_DEV)
        return reduce_density(window, occupations, domains, lax.axis_size("band"))
    return ring_density(wavefunctions, projectors, slot_ids, occupations)


def solution(mesh):
    in_specs = (P("band", "grid"), P("grid", None, None, None), P("grid", None), P("band"))
    out_specs = P("grid", None, None)
    return jax.shard_map(body, mesh=mesh, in_specs=in_specs, out_specs=out_specs, check_vma=False)
```

```python
import functools

import jax
import jax.numpy as jnp
from jax import lax
from jax.experimental import pallas as pl
from jax.experimental.pallas import tpu as pltpu
from jax.sharding import PartitionSpec as P

REACH = 3
ATOMS_DEV = 32
ROWS = 8
LANES = 128
STRIDE = 16
SKEW = 3
STEP_BLOCKS = 8
MESH = pl.DeviceIdType.MESH
HIGHEST = lax.Precision.HIGHEST


def nt_dot(a, b, precision=None):
    return lax.dot_general(
        a, b, (((1,), (1,)), ((), ())), precision=precision, preferred_element_type=jnp.float32
    )


def split(full):
    high = full.astype(jnp.bfloat16)
    return high, (full - high.astype(jnp.float32)).astype(jnp.bfloat16)


def local_kernel(ids_ref, waves_ref, pieces_ref, out_ref, slots):
    step = pl.program_id(0)
    per_step, proj_count, capacity, block_len = pieces_ref.shape
    bands = waves_ref.shape[0]
    halves, _, targets, lanes = out_ref.shape
    for g in range(per_step):
        stacked = pieces_ref[g].reshape(proj_count * capacity, block_len)
        terms = nt_dot(stacked, waves_ref[:, g * block_len:(g + 1) * block_len])
        start = pl.multiple_of((step * per_step + g) * capacity, capacity)
        for i in range(proj_count):
            slots[pl.ds(start, capacity), i * bands:(i + 1) * bands] = terms[i * capacity:(i + 1) * capacity]

    @pl.when(step == pl.num_programs(0) - 1)
    def _():
        slot_count = slots.shape[0]
        wanted = lax.broadcasted_iota(jnp.int32, (targets, slot_count), 0)
        pick = (wanted == ids_ref[...]).astype(jnp.bfloat16)
        for i in range(proj_count):
            full = slots[:, i * bands:(i + 1) * bands]
            high, low = split(full)
            total = jnp.dot(pick, high, preferred_element_type=jnp.float32)
            total += jnp.dot(pick, low, preferred_element_type=jnp.float32)
            for h in range(halves):
                out_ref[h, i] = total[:, h * lanes:(h + 1) * lanes]


def local_window(wavefunctions, projectors, slot_ids, targets):
    bands = wavefunctions.shape[0]
    blocks, capacity, proj_count, block_len = projectors.shape
    shape = (bands // LANES, proj_count, targets, LANES)
    return pl.pallas_call(
        local_kernel,
        grid=(blocks // STEP_BLOCKS,),
        in_specs=[
            pl.BlockSpec((1, blocks * capacity), lambda s: (0, 0)),
            pl.BlockSpec((bands, STEP_BLOCKS * block_len), lambda s: (0, s)),
            pl.BlockSpec((STEP_BLOCKS, proj_count, capacity, block_len), lambda s: (s, 0, 0, 0)),
        ],
        out_specs=pl.BlockSpec(shape, lambda s: (0, 0, 0, 0)),
        out_shape=jax.ShapeDtypeStruct(shape, jnp.float32),
        scratch_shapes=[
            pltpu.VMEM((blocks * capacity, proj_count * bands), jnp.float32),
        ],
        compiler_params=pltpu.CompilerParams(vmem_limit_bytes=60 << 20),
    )(slot_ids.reshape(1, -1), wavefunctions, projectors.transpose(0, 2, 1, 3))


def reduce_kernel(groups, band_size, win, occ, out_ref, pair_in, hop_in, summed, mine, peers, final, landed,
                  pair_send, pair_recv, hop_send, hop_recv, peer_send, peer_recv, last_send, last_recv):
    halves, proj_count, _, lanes = win.shape
    band = lax.axis_index("band")
    domain = lax.axis_index("grid")
    core = domain % 2
    chip = domain // 2
    chips = groups // 2
    turns = chips // 2
    subs = ATOMS_DEV // ROWS
    per_turn = subs * halves
    chunks = turns * per_turn
    top = (proj_count + 1) // 2 * ROWS
    rows = proj_count * ROWS

    barrier = pltpu.get_barrier_semaphore()
    partner = (band, chip * 2 + 1 - core)
    met = [partner]
    for r in range(1, chips):
        met.append((band, ((chip + r) % chips) * 2 + core))
    for r in range(1, band_size):
        met.append(((band + r) % band_size, domain))
    for other in met:
        pl.semaphore_signal(barrier, inc=1, device_id=other, device_id_type=MESH)

    def place(direction, k):
        block = k // halves
        turn = block // subs
        owner = turns - 1 - turn if direction == 0 else turns + turn
        return k % halves, pl.multiple_of(block * ROWS, ROWS), owner, block % subs

    def pair_copy(direction, k):
        half, at, owner, sub = place(direction, k)
        source = pl.multiple_of((owner * 2 + 1 - core) * ATOMS_DEV + sub * ROWS, ROWS)
        return pltpu.make_async_remote_copy(
            src_ref=win.at[half, :, pl.ds(source, ROWS), :],
            dst_ref=pair_in.at[direction, half, :, pl.ds(at, ROWS), :],
            send_sem=pair_send.at[direction, k], recv_sem=pair_recv.at[direction, k],
            device_id=partner, device_id_type=MESH,
        )

    def hop_copy(direction, k):
        half, at, _, _ = place(direction, k)
        following = chip - 1 if direction == 0 else chip + 1
        return pltpu.make_async_remote_copy(
            src_ref=summed.at[direction, half, :, pl.ds(at, ROWS), :],
            dst_ref=hop_in.at[direction, half, :, pl.ds(at, ROWS), :],
            send_sem=hop_send.at[direction, k], recv_sem=hop_recv.at[direction, k],
            device_id=(band, following * 2 + core), device_id_type=MESH,
        )

    def peer_copy(turn, r):
        return pltpu.make_async_remote_copy(
            src_ref=mine.at[turn], dst_ref=peers.at[turn, r - 1],
            send_sem=peer_send.at[turn, r - 1], recv_sem=peer_recv.at[turn, r - 1],
            device_id=((band + r) % band_size, domain), device_id_type=MESH,
        )

    def last_copy(direction, turn):
        owner = turns - 1 - turn if direction == 0 else turns + turn
        return pltpu.make_async_remote_copy(
            src_ref=final.at[turn], dst_ref=landed,
            send_sem=last_send.at[turn], recv_sem=last_recv,
            device_id=(band, owner * 2 + core), device_id_type=MESH,
        )

    def summed_peers(turn):
        total = mine[turn]
        for r in range(1, band_size):
            peer_copy(turn, r).wait_recv()
            total = total + peers[turn, r - 1]
        return total

    mine[...] = jnp.zeros_like(mine)
    pl.semaphore_wait(barrier, len(met))

    @pl.loop(0, chunks)
    def _(k):
        for direction in range(2):
            pair_copy(direction, k).start()

    def density(direction, k):
        _, at, _, sub = place(direction, k)

        @pl.when(k % halves == halves - 1)
        def _():
            x = [summed[direction, h, :, pl.ds(at, ROWS), :].reshape(rows, lanes) for h in range(halves)]
            left = split(jnp.concatenate([x[h] * occ[h] for h in range(halves)], axis=1))
            right = split(jnp.concatenate(x, axis=1))
            gram = nt_dot(left[0], right[0]) + nt_dot(left[0], right[1]) + nt_dot(left[1], right[0])
            r = lax.broadcasted_iota(jnp.int32, (rows, rows), 0)
            c = lax.broadcasted_iota(jnp.int32, (rows, rows), 1)
            gram = split(jnp.where(r % ROWS == c % ROWS, gram, 0.0))
            j = lax.broadcasted_iota(jnp.int32, (rows, LANES), 0) // ROWS
            lane = lax.broadcasted_iota(jnp.int32, (rows, LANES), 1)
            gather = (lane % (subs * STRIDE) == sub * STRIDE + j).astype(jnp.bfloat16)
            packed = jnp.dot(gram[0], gather, preferred_element_type=jnp.float32)
            packed += jnp.dot(gram[1], gather, preferred_element_type=jnp.float32)
            turn = k // per_turn
            low_lane = lane < subs * STRIDE
            mine[turn, :, :] += jnp.where(low_lane[:top], packed[:top], 0.0)
            mine[turn, :rows - top, :] += jnp.where(low_lane[top:], 0.0, packed[top:])

        for turn in range(turns):
            @pl.when(k == (turn + 1) * per_turn - 1)
            def _():
                for r in range(1, band_size):
                    peer_copy(turn, r).start()
        for turn in range(turns - 1):
            @pl.when(k == (turn + 1) * per_turn - 1 + per_turn // 2)
            def _():
                final[turn] = summed_peers(turn)
                last_copy(direction, turn).start()

    def process(direction, k, hops):
        half, at, owner, sub = place(direction, k)
        source = pl.multiple_of((owner * 2 + core) * ATOMS_DEV + sub * ROWS, ROWS)
        here = (direction, half, slice(None), pl.ds(at, ROWS), slice(None))
        pair_copy(direction, k).wait_recv()
        summed[here] = win[half, :, pl.ds(source, ROWS), :] + pair_in[here]

        @pl.when(hops > 0)
        def _():
            hop_copy(direction, k).wait_recv()
            summed[here] = summed[here] + hop_in[here]

        @pl.when(hops < chips - 1)
        def _():
            hop_copy(direction, k).start()

        @pl.when(hops == chips - 1)
        def _():
            density(direction, k)

    @pl.loop(0, chunks + SKEW * (chips - 1))
    def _(t):
        for direction in range(2):
            hops = chips - 1 - chip if direction == 0 else chip
            k = t - SKEW * hops

            @pl.when((k >= 0) & (k < chunks))
            def _():
                process(direction, k, hops)

    edge = (chip == 0) | (chip == chips - 1)

    @pl.when(edge)
    def _():
        out_ref[...] = summed_peers(turns - 1)
        for turn in range(turns):
            for r in range(1, band_size):
                peer_copy(turn, r).wait_send()
        for turn in range(turns - 1):
            last_copy(0, turn).wait_send()

    @pl.when(jnp.logical_not(edge))
    def _():
        last_copy(0, 0).wait_recv()
        out_ref[...] = landed[...]

    @pl.loop(0, chunks)
    def _(k):
        for direction in range(2):
            hops = chips - 1 - chip if direction == 0 else chip
            pair_copy(direction, k).wait_send()

            @pl.when(hops < chips - 1)
            def _():
                hop_copy(direction, k).wait_send()


def reduce_density(window, occupations, groups, band_size):
    halves, proj_count, _, lanes = window.shape
    turns = groups // 4
    chunks = turns * ATOMS_DEV // ROWS * halves
    top = (proj_count + 1) // 2 * ROWS
    handled = (2, halves, proj_count, turns * ATOMS_DEV, lanes)
    vmem = pl.BlockSpec(memory_space=pltpu.VMEM)
    dma = pltpu.SemaphoreType.DMA
    packed = pl.pallas_call(
        functools.partial(reduce_kernel, groups, band_size),
        in_specs=[vmem, vmem],
        out_specs=vmem,
        out_shape=jax.ShapeDtypeStruct((top, LANES), jnp.float32),
        scratch_shapes=[
            pltpu.VMEM(handled, jnp.float32),
            pltpu.VMEM(handled, jnp.float32),
            pltpu.VMEM(handled, jnp.float32),
            pltpu.VMEM((turns, top, LANES), jnp.float32),
            pltpu.VMEM((turns, band_size - 1, top, LANES), jnp.float32),
            pltpu.VMEM((turns, top, LANES), jnp.float32),
            pltpu.VMEM((top, LANES), jnp.float32),
            dma((2, chunks)), dma((2, chunks)), dma((2, chunks)), dma((2, chunks)),
            dma((turns, band_size - 1)), dma((turns, band_size - 1)), dma((turns,)), dma,
        ],
        compiler_params=pltpu.CompilerParams(
            collective_id=0, has_side_effects=True, vmem_limit_bytes=40 << 20
        ),
    )(window, occupations.reshape(halves, 1, lanes))
    subs = ATOMS_DEV // ROWS
    packed = packed.reshape(top // ROWS, ROWS, 2, subs, STRIDE).transpose(3, 1, 2, 0, 4)
    packed = packed.reshape(ATOMS_DEV, 2 * top // ROWS, STRIDE)
    return packed[:, :proj_count, :proj_count]


def shifted(block, axis, distance):
    devices = range(lax.axis_size(axis))
    route = [((i - distance) % len(devices), i) for i in devices]
    return lax.ppermute(block, axis, route)


def ring_density(wavefunctions, projectors, slot_ids, occupations):
    domains = lax.axis_size("grid")
    domain = lax.axis_index("grid")
    window_len = 2 * REACH + 1
    owner = jnp.floor_divide(slot_ids, ATOMS_DEV)
    offset = jnp.mod(owner - domain + REACH, domains)
    target = jnp.where(slot_ids >= 0, offset * ATOMS_DEV + jnp.mod(slot_ids, ATOMS_DEV), -1)
    window = local_window(wavefunctions, projectors, target, window_len * ATOMS_DEV)
    halves, proj_count, _, lanes = window.shape
    window = window.reshape(halves, proj_count, window_len, ATOMS_DEV, lanes)
    part = lambda at: window[:, :, at]
    forward = part(2 * REACH)
    for hop in range(REACH, 0, -1):
        forward = shifted(forward, "grid", 1) + part(REACH + hop - 1)
    backward = part(0)
    for hop in range(REACH, 0, -1):
        backward = shifted(backward, "grid", -1)
        if hop > 1:
            backward = backward + part(REACH - hop + 1)
    owned = forward + backward
    weighted = owned * occupations.reshape(halves, 1, 1, lanes)
    partial_sum = jnp.einsum("hian,hjan->aij", weighted, owned, precision=HIGHEST)
    return lax.psum(partial_sum, "band")


def body(wavefunctions, projectors, slot_atom, occupations):
    domains = lax.axis_size("grid")
    slot_ids = slot_atom.reshape(-1)
    if domains <= 2 * REACH + 2 and domains % 4 == 0:
        window = local_window(wavefunctions, projectors, slot_ids, domains * ATOMS_DEV)
        return reduce_density(window, occupations, domains, lax.axis_size("band"))
    return ring_density(wavefunctions, projectors, slot_ids, occupations)


def solution(mesh):
    in_specs = (P("band", "grid"), P("grid", None, None, None), P("grid", None), P("band"))
    out_specs = P("grid", None, None)
    return jax.shard_map(body, mesh=mesh, in_specs=in_specs, out_specs=out_specs, check_vma=False)
```
